32 devices in a mesh: seq: 8 (over z, core), mp: 4 (over y, x).
Axes of the slice: x: 2, y: 2, z: 4, core: 2. Of those that a mesh axis runs over, the one named last changes fastest.
Arguments:
- hidden_in: bfloat16 [4096, 4096], P('seq', 'mp'), may hold values from -30 to 30
- norm_gain: float32 [4096], replicated, may hold values from 0.1 to 1.9
- w_z: bfloat16 [4096, 8192], P('seq', 'mp'), may hold values from -0.09375 to 0.09375
- w_x: bfloat16 [4096, 8192], P('seq', 'mp'), may hold values from -0.09375 to 0.09375
- w_b: bfloat16 [4096, 1024], P('seq', 'mp'), may hold values from -0.09375 to 0.09375
- w_c: bfloat16 [4096, 1024], P('seq', 'mp'), may hold values from -0.09375 to 0.09375
- w_dt: bfloat16 [4096, 128], P('seq', 'mp'), may hold values from -0.0625 to 0.0625
- conv_x: float32 [4, 8192], P(None, 'mp'), may hold values from -3 to 3
- conv_b: float32 [4, 1024], P(None, 'mp'), may hold values from -3 to 3
- conv_c: float32 [4, 1024], P(None, 'mp'), may hold values from -3 to 3
- dt_bias: float32 [128], P('mp'), may hold values from -9 to -5
- a_rate: float32 [128], P('mp'), may hold values from 0.5 to 16
- skip_gain: float32 [128], P('mp'), may hold values from -3 to 3
- group_gain: float32 [8192], P('mp'), may hold values from 0.1 to 1.9
- w_out: bfloat16 [8192, 4096], P('mp', 'seq'), may hold values from -0.0625 to 0.0625
- attn_gain: float32 [4096], replicated, may hold values from 0.1 to 1.9
- w_q: bfloat16 [4096, 4096], P(None, 'mp'), may hold values from -0.125 to 0.125
- w_k: bfloat16 [4096, 1024], P(None, 'mp'), may hold values from -0.125 to 0.125
- w_v: bfloat16 [4096, 1024], P(None, 'mp'), may hold values from -0.09375 to 0.09375
Outputs:
- mixed: float32 [4096, 4096], P('seq', 'mp')
- context: float32 [4096, 4096], P('seq', 'mp')
The draws below stay inside these ranges and needn't reach their ends.
All inputs are finite; a program needn't handle non-finite values.
Results may differ from the reference program's by a relative error of at most 0.017.
Values may be sent and summed in bfloat16 or wider, within the bound.
A program may use at most 192 MiB of HBM per device.

```python
import math
import jax
import jax.numpy as jnp
from jax import lax

D = 4096
DI = 8192
H = 128
P_SIZE = 64
N = 128
G = 8
KW = 4
HQ = 32
HK = 8
HD = 128
WINDOW = 4096
QB = 128
TOK_DEV = 512
TOKENS = 4096
N_SEQ = 8
N_MP = 4


def contiguous_spans(key):
    forward_sense = jnp.clip(jax.random.normal(jax.random.fold_in(key, 101), (D,), jnp.float32), -4.0, 4.0)
    processor_slots = jax.random.randint(jax.random.fold_in(key, 102), (TOKENS // TOK_DEV * 2,), 0, TOKENS)
    input_magnitude = jax.random.uniform(jax.random.fold_in(key, 103), (TOKENS // TOK_DEV * 2,), jnp.float32, 0.6, 1.0)
    return (forward_sense, processor_slots, input_magnitude)


def draw_hidden_in(key, part):
    forward_sense, processor_slots, input_magnitude = contiguous_spans(key)
    base = jnp.clip(jax.random.normal(jax.random.fold_in(key, 1), (TOKENS, D), jnp.float32), -6.0, 6.0)
    mixing = jnp.zeros((TOKENS,), jnp.float32).at[processor_slots].set(input_magnitude)
    values = base * (1.0 - mixing)[:, None] + forward_sense[None, :] * (4.0 * mixing)[:, None]
    return jnp.clip(values, -30.0, 30.0).astype(jnp.bfloat16)


def draw_w_dt(key, part):
    forward_sense, processor_slots, input_magnitude = contiguous_spans(key)
    noise = 0.3 * jnp.clip(jax.random.normal(jax.random.fold_in(key, 3), (D, H), jnp.float32), -6.0, 6.0) / math.sqrt(D)
    lifted = jax.random.uniform(jax.random.fold_in(key, 4), (H,), jnp.float32, 6.0, 10.0)
    limit = 4.0 / math.sqrt(D)
    return jnp.clip(noise + forward_sense[:, None] * lifted[None, :] / D, -limit, limit).astype(jnp.bfloat16)


def draw_w_q(key, part):
    base = jnp.clip(jax.random.normal(jax.random.fold_in(key, 5), (D, HQ * HD), jnp.float32), -6.0, 6.0) / math.sqrt(D)
    limit = 8.0 / math.sqrt(D)
    return jnp.clip(base, -limit, limit).astype(jnp.bfloat16)


def draw_w_k(key, part):
    base = jnp.clip(jax.random.normal(jax.random.fold_in(key, 6), (D, HK * HD), jnp.float32), -6.0, 6.0) / math.sqrt(D)
    limit = 8.0 / math.sqrt(D)
    return jnp.clip(base, -limit, limit).astype(jnp.bfloat16)


def block_levels(own_key, dims, split, smallest, largest):
    factor_of, own = 1.0, jax.random.fold_in(own_key, 6)
    for position, blocks in split:
        draws = jnp.exp(jax.random.uniform(jax.random.fold_in(own, position), (blocks,), jnp.float32, smallest / len(split), largest / len(split)))
        factor_of = factor_of * jnp.repeat(draws, dims[position] // blocks).reshape([-1 if axis == position else 1 for axis in range(len(dims))])
    return factor_of


def scatter_about(own_key, dims, scale, bound, split=(), kind=jnp.bfloat16):
    result = scale * jax.random.normal(own_key, dims, jnp.float32)
    if split:
        result = result * block_levels(own_key, dims, split, -0.22, 0.18)
    return jnp.clip(result, -bound, bound).astype(kind)


def setup_inputs(seed: int = 0) -> dict:
    key_list = jax.random.split(jax.random.key(seed), 20)
    return {
        "hidden_in": draw_hidden_in(jax.random.fold_in(key_list[19], 71), 0),
        "norm_gain": jnp.clip(1.0 + 0.18 * jax.random.normal(key_list[1], (D,), jnp.float32), 0.1, 1.9),
        "w_z": scatter_about(key_list[2], (D, DI), D ** -0.5, 0.09375, ((0, 8), (1, 4))),
        "w_x": scatter_about(key_list[3], (D, DI), D ** -0.5, 0.09375, ((0, 8), (1, 4))),
        "w_b": scatter_about(key_list[4], (D, G * N), D ** -0.5, 0.09375, ((0, 8), (1, 4))),
        "w_c": scatter_about(key_list[5], (D, G * N), D ** -0.5, 0.09375, ((0, 8), (1, 4))),
        "w_dt": draw_w_dt(jax.random.fold_in(key_list[19], 71), 0),
        "conv_x": scatter_about(key_list[7], (KW, DI), 0.5, 3.0, ((1, 4),), jnp.float32),
        "conv_b": scatter_about(key_list[8], (KW, G * N), 0.5, 3.0, ((1, 4),), jnp.float32),
        "conv_c": scatter_about(key_list[9], (KW, G * N), 0.5, 3.0, ((1, 4),), jnp.float32),
        "dt_bias": jnp.clip(-9.0 + 4.0 * jax.random.uniform(key_list[10], (H,), jnp.float32) ** block_levels(key_list[10], (H,), ((0, 4),), -0.2, 0.2), -9.0, -5.0),
        "a_rate": jnp.clip(jnp.exp(math.log(16.0) - 3.465736 * jax.random.uniform(key_list[11], (H,), jnp.float32) ** block_levels(key_list[11], (H,), ((0, 4),), -0.2, 0.2)), 0.5, 16.0),
        "skip_gain": scatter_about(key_list[12], (H,), 1.0, 3.0, ((0, 4),), jnp.float32),
        "group_gain": jnp.clip(1.0 + 0.18 * jax.random.normal(key_list[13], (DI,), jnp.float32), 0.1, 1.9),
        "w_out": scatter_about(key_list[14], (DI, D), DI ** -0.5, 0.0625, ((0, 4), (1, 8))),
        "attn_gain": jnp.clip(1.0 + 0.18 * jax.random.normal(key_list[15], (D,), jnp.float32), 0.1, 1.9),
        "w_q": draw_w_q(jax.random.fold_in(key_list[19], 71), 0),
        "w_k": draw_w_k(jax.random.fold_in(key_list[19], 71), 0),
        "w_v": scatter_about(key_list[18], (D, HK * HD), D ** -0.5, 0.09375, ((1, 4),)),
    }


HIGH = lax.Precision.HIGHEST

def rms_norm(values, gain):
    return values * lax.rsqrt(lax.optimization_barrier(jnp.mean(values * values, axis=-1, keepdims=True)) + 1e-05) * gain

def causal_conv(values, rim, device_routine):
    padded = jnp.concatenate([rim, values], axis=0)
    length = values.shape[0]
    summed = jnp.zeros(values.shape, jnp.float32)
    for offset in range(device_routine.shape[0]):
        summed = summed + device_routine[offset][None, :] * padded[offset:offset + length]
    return jax.nn.silu(summed)

def ssd_block(carry_state, pieces):
    inputs, step_sizes, decays, keys_b, reads_c = pieces
    per_group = inputs.shape[1] // keys_b.shape[1]
    b_heads = jnp.repeat(keys_b, per_group, axis=1)
    c_heads = jnp.repeat(reads_c, per_group, axis=1)
    cumulative = jnp.cumsum(decays, axis=0)
    length = inputs.shape[0]
    causal_mask = jnp.arange(length)[:, None] >= jnp.arange(length)[None, :]
    spread = cumulative[:, None, :] - cumulative[None, :, :]
    within = jnp.exp(jnp.where(causal_mask[:, :, None], spread, -jnp.inf))
    affinity = jnp.einsum('tgn,sgn->gts', reads_c, keys_b, precision=HIGH)
    affinity = jnp.repeat(affinity, per_group, axis=0)
    mixing = affinity * jnp.transpose(within, (2, 0, 1)) * jnp.transpose(step_sizes)[:, None, :]
    inside = jnp.einsum('hts,shp->thp', mixing, inputs, precision=HIGH)
    carried = jnp.exp(cumulative)[:, :, None] * jnp.einsum('thn,hpn->thp', c_heads, carry_state, precision=HIGH)
    tail_weight = jnp.exp(cumulative[-1][None, :] - cumulative) * step_sizes
    fresh_state = jnp.einsum('sh,shp,shn->hpn', tail_weight, inputs, b_heads, precision=HIGH)
    updated = jnp.exp(cumulative[-1])[:, None, None] * carry_state + fresh_state
    return (updated, inside + carried)

def run_ssd(inputs, step_sizes, decays, keys_b, reads_c, block, carry_state):
    total_rows = inputs.shape[0]
    block_count = total_rows // block

    def blocked(values):
        return values.reshape((block_count, block) + values.shape[1:])
    final_state, outputs = lax.scan(ssd_block, carry_state, (blocked(inputs), blocked(step_sizes), blocked(decays), blocked(keys_b), blocked(reads_c)))
    return (final_state, outputs.reshape((total_rows,) + outputs.shape[2:]))

def window_attention(asking_vectors, keys, values, shift_rows, first_key):
    per_kv = asking_vectors.shape[1] // keys.shape[1]
    keys_all = jnp.repeat(keys, per_kv, axis=1)
    values_all = jnp.repeat(values, per_kv, axis=1)
    query_rows = asking_vectors.shape[0]
    key_count = keys.shape[0]
    scale = asking_vectors.shape[2] ** (-0.5)
    index_offsets = jnp.arange(key_count)[None, :] - shift_rows - jnp.arange(query_rows)[:, None]
    allowed = (index_offsets <= 0) & (index_offsets > -WINDOW) & (first_key + jnp.arange(key_count) >= 0)[None, :]

    def one_head(operands):
        query_h, key_h, value_h = operands
        scores = lax.dot_general(query_h, key_h, (((1,), (1,)), ((), ())), preferred_element_type=jnp.float32) * scale
        scores = jnp.where(allowed, scores, -jnp.inf)
        row_peak = lax.optimization_barrier(jnp.max(scores, axis=1, keepdims=True))
        exp_scores = jnp.exp(scores - row_peak)
        weights = (exp_scores / lax.optimization_barrier(jnp.sum(exp_scores, axis=1, keepdims=True))).astype(jnp.bfloat16)
        return jnp.dot(weights, value_h, preferred_element_type=jnp.float32)
    outputs = lax.map(one_head, (jnp.transpose(asking_vectors, (1, 0, 2)), jnp.transpose(keys_all, (1, 0, 2)), jnp.transpose(values_all, (1, 0, 2))))
    return jnp.transpose(outputs, (1, 0, 2)).reshape(query_rows, -1)

def reference(hidden_in, norm_gain, w_z, w_x, w_b, w_c, w_dt, conv_x, conv_b, conv_c, dt_bias, a_rate, skip_gain, group_gain, w_out, attn_gain, w_q, w_k, w_v):
    stream = hidden_in.astype(jnp.float32)
    normed = rms_norm(stream, norm_gain).astype(jnp.bfloat16)
    gate_proj = jnp.dot(normed, w_z, preferred_element_type=jnp.float32)
    input_mapped = jnp.dot(normed, w_x, preferred_element_type=jnp.float32)
    b_proj = jnp.dot(normed, w_b, preferred_element_type=jnp.float32)
    c_proj = jnp.dot(normed, w_c, preferred_element_type=jnp.float32)
    delta_time_unscaled = jnp.dot(normed, w_dt, preferred_element_type=jnp.float32)
    conv_in = causal_conv(input_mapped, jnp.zeros((KW - 1, DI), jnp.float32), conv_x)
    conv_bv = causal_conv(b_proj, jnp.zeros((KW - 1, G * N), jnp.float32), conv_b)
    conv_cv = causal_conv(c_proj, jnp.zeros((KW - 1, G * N), jnp.float32), conv_c)
    step_sizes = jax.nn.softplus(delta_time_unscaled + dt_bias[None, :])
    decays = -a_rate[None, :] * step_sizes
    inputs = conv_in.reshape(TOKENS, H, P_SIZE)
    final_state, ssd_out = run_ssd(inputs, step_sizes, decays, conv_bv.reshape(TOKENS, G, N), conv_cv.reshape(TOKENS, G, N), QB, jnp.zeros((H, P_SIZE, N), jnp.float32))
    full = ssd_out + skip_gain[None, :, None] * inputs
    gated = full.reshape(TOKENS, DI) * jax.nn.silu(gate_proj)
    grouped = gated.reshape(TOKENS, G, DI // G)
    y_normed = rms_norm(grouped, group_gain.reshape(G, DI // G)).reshape(TOKENS, DI).astype(jnp.bfloat16)
    width = DI // N_MP
    summed = jnp.zeros((TOKENS, D), jnp.float32)
    for member in range(N_MP):
        term = jnp.dot(y_normed[:, member * width:(member + 1) * width], w_out[member * width:(member + 1) * width], preferred_element_type=jnp.float32)
        summed = summed + lax.optimization_barrier(term.astype(jnp.bfloat16)).astype(jnp.float32)
    mixed = stream + summed
    mixed_low = lax.optimization_barrier(mixed.astype(jnp.bfloat16)).astype(jnp.float32)
    normed_two = rms_norm(mixed_low, attn_gain).astype(jnp.bfloat16)
    asking_vectors = jnp.dot(normed_two, w_q, preferred_element_type=jnp.float32).astype(jnp.bfloat16).reshape(TOKENS, HQ, HD)
    keys = jnp.dot(normed_two, w_k, preferred_element_type=jnp.float32).astype(jnp.bfloat16).reshape(TOKENS, HK, HD)
    values = jnp.dot(normed_two, w_v, preferred_element_type=jnp.float32).astype(jnp.bfloat16).reshape(TOKENS, HK, HD)
    keys_pad = jnp.concatenate([jnp.zeros((WINDOW, HK, HD), jnp.bfloat16), keys], axis=0)
    values_pad = jnp.concatenate([jnp.zeros((WINDOW, HK, HD), jnp.bfloat16), values], axis=0)

    def one_block(block_index):
        start = (block_index * TOK_DEV).astype(jnp.int32)
        asking_tile = lax.dynamic_slice_in_dim(asking_vectors, start, TOK_DEV, 0)
        key_blk = lax.dynamic_slice_in_dim(keys_pad, start, WINDOW + TOK_DEV, 0)
        value_blk = lax.dynamic_slice_in_dim(values_pad, start, WINDOW + TOK_DEV, 0)
        return window_attention(asking_tile, key_blk, value_blk, WINDOW, start - WINDOW)
    blocks = lax.map(one_block, jnp.arange(N_SEQ, dtype=jnp.int32))
    context = blocks.reshape(TOKENS, HQ * HD)
    return (mixed, context)
```

```python
import functools
import math

import jax
import jax.numpy as jnp
from jax import lax
from jax.experimental import pallas as pl
from jax.experimental.pallas import tpu as pltpu
from jax.sharding import PartitionSpec as P

P_SIZE = 64
N = 128
HD = 128
WINDOW = 4096
QB = 128
LANES = 128
VMEM_LIMIT = 62 * 1024 * 1024

HIGH = lax.Precision.HIGHEST
F32 = jnp.float32
BF16 = jnp.bfloat16


def from_behind(block, axis, distance):
    devices = range(lax.axis_size(axis))
    route = [(i - distance, i) for i in devices if i - distance in devices]
    return lax.ppermute(block, axis, route)


def rms_norm(values, gain):
    return values * lax.rsqrt(jnp.mean(values * values, axis=-1, keepdims=True) + 1e-05) * gain


def signal_seq(sem, index):
    pl.semaphore_signal(
        sem, inc=1, device_id={"seq": index}, device_id_type=pl.DeviceIdType.MESH
    )


def gather_dot_kernel(n, normed_ref, w_ref, out_ref, slots, local_sem, send_sem, recv_sem):
    me = lax.axis_index("seq")
    ring = n // 2
    half = ring // 2
    chip, core = me // 2, lax.rem(me, 2)
    up = lax.rem(chip + 1, ring) * 2 + core
    down = lax.rem(chip + ring - 1, ring) * 2 + core
    partner = chip * 2 + 1 - core
    depth, cols = w_ref.shape
    mid = depth // 2

    barrier = pltpu.get_barrier_semaphore()
    for other in (up, down, partner):
        signal_seq(barrier, other)
    pl.semaphore_wait(barrier, 3)

    local = pltpu.make_async_copy(w_ref, slots.at[0], local_sem)
    local.start()
    started = []

    def send(source, slot, rows, part, target):
        copy = pltpu.make_async_remote_copy(
            src_ref=source,
            dst_ref=slots.at[slot, rows],
            send_sem=send_sem.at[len(started)],
            recv_sem=recv_sem.at[2 * slot + part],
            device_id={"seq": target},
            device_id_type=pl.DeviceIdType.MESH,
        )
        copy.start()
        started.append(copy)

    def arrived(slot, rows, part):
        pltpu.make_async_copy(
            slots.at[slot, rows], slots.at[slot, rows], recv_sem.at[2 * slot + part]
        ).wait()

    whole, upper, lower = pl.ds(0, depth), pl.ds(0, mid), pl.ds(mid, mid)
    send(w_ref, 2 * 1, whole, 0, up)
    send(w_ref, 2 * (ring - 1), whole, 0, down)
    send(w_ref, 1, whole, 0, partner)

    def multiply(slot, first=False):
        step, lane = slot // 2, slot % 2
        origin = lax.rem(chip - step + ring, ring) * 2
        owner = origin + (core if lane == 0 else 1 - core)
        features = pl.ds(pl.multiple_of(owner * depth, depth), depth)

        def tile(start, width):
            where = pl.ds(start, width)
            product = jnp.dot(
                normed_ref[:, features], slots[slot, :, where], preferred_element_type=F32
            )
            if first:
                out_ref[:, where] = product
            else:
                out_ref[:, where] += product

        width = 512
        full = cols // width

        def body(i, carry):
            tile(pl.multiple_of(i * width, width), width)
            return carry

        lax.fori_loop(0, full, body, 0)
        if cols % width:
            tile(full * width, cols % width)

    local.wait()
    multiply(0, True)
    arrived(1, whole, 0)
    multiply(1)
    for d in range(1, half):
        s_up, s_down = 2 * d, 2 * (ring - d)
        last = d + 1 == half
        arrived(s_up, whole, 0)
        rows = upper if last else whole
        send(slots.at[s_up, rows], 2 * (d + 1), rows, 0, up)
        arrived(s_down, whole, 0)
        rows = lower if last else whole
        send(slots.at[s_down, rows], 2 * (ring - d - 1), rows, 1 if last else 0, down)
        send(slots.at[s_up, whole], s_up + 1, whole, 0, partner)
        send(slots.at[s_down, whole], s_down + 1, whole, 0, partner)
        multiply(s_up)
        multiply(s_down)
        arrived(s_up + 1, whole, 0)
        multiply(s_up + 1)
        arrived(s_down + 1, whole, 0)
        multiply(s_down + 1)
    far = 2 * half
    arrived(far, upper, 0)
    send(slots.at[far, upper], far + 1, upper, 0, partner)
    arrived(far, lower, 1)
    send(slots.at[far, lower], far + 1, lower, 1, partner)
    multiply(far)
    arrived(far + 1, upper, 0)
    arrived(far + 1, lower, 1)
    multiply(far + 1)
    for copy in started:
        copy.wait_send()


def gather_dot(normed, weights):
    n = lax.axis_size("seq")
    depth, cols = weights.shape
    ring = n // 2
    sends = 3 + 4 * (ring // 2 - 1) + 2
    return pl.pallas_call(
        functools.partial(gather_dot_kernel, n),
        out_shape=jax.ShapeDtypeStruct((normed.shape[0], cols), F32),
        in_specs=[
            pl.BlockSpec(memory_space=pltpu.VMEM),
            pl.BlockSpec(memory_space=pl.ANY),
        ],
        out_specs=pl.BlockSpec(memory_space=pltpu.VMEM),
        scratch_shapes=[
            pltpu.VMEM((n, depth, cols), BF16),
            pltpu.SemaphoreType.DMA,
            pltpu.SemaphoreType.DMA((sends,)),
            pltpu.SemaphoreType.DMA((2 * n,)),
        ],
        compiler_params=pltpu.CompilerParams(
            collective_id=0, has_side_effects=True, vmem_limit_bytes=VMEM_LIMIT
        ),
        cost_estimate=pl.CostEstimate(
            flops=2 * normed.shape[0] * normed.shape[1] * cols,
            bytes_accessed=160_000_000,
            transcendentals=0,
        ),
    )(normed, weights)


def silu(v):
    return v / (1.0 + jnp.exp(-v))


def spread_heads(values, expand):
    high = values.astype(BF16)
    low = (values - high.astype(F32)).astype(BF16)
    return jnp.dot(high, expand, preferred_element_type=F32) + jnp.dot(
        low, expand, preferred_element_type=F32
    )


def mixer_kernel(
    n,
    heads,
    groups,
    proj_ref,
    rim_ref,
    taps_ref,
    bias_ref,
    rate_ref,
    skip_ref,
    gain_ref,
    expand_ref,
    y_ref,
    window,
    conv,
    ssd,
    reads,
    logs,
    state,
    carry,
    state_out,
    carry_out,
    state_in,
    carry_in,
    send_sem,
    recv_sem,
):
    me = lax.axis_index("seq")
    rows = proj_ref.shape[0]
    inner = heads * P_SIZE
    width = inner + 2 * groups * N
    gate_at = width + LANES
    per_group = inner // groups
    blocks = rows // QB
    kw = taps_ref.shape[0]

    barrier = pltpu.get_barrier_semaphore()
    for d in range(1, n):
        signal_seq(barrier, lax.rem(me + d, n))
    pl.semaphore_wait(barrier, n - 1)

    expand = expand_ref[...]
    window[0:8, :] = rim_ref[...]
    state[...] = jnp.zeros_like(state)
    carry[...] = jnp.zeros_like(carry)
    row_id = lax.broadcasted_iota(jnp.int32, (QB, QB), 0)
    col_id = lax.broadcasted_iota(jnp.int32, (QB, QB), 1)
    causal = row_id >= col_id
    low_lanes = col_id < P_SIZE
    tri = jnp.where(causal, 1.0, 0.0).astype(F32)

    def block(i, carry_none):
        base = pl.multiple_of(i * QB, QB)
        here = pl.ds(base, QB)
        window[8 : 8 + QB, :] = proj_ref[here, 0:width]
        step_cols = 256 if width % 256 == 0 else 128
        for at in range(0, width, step_cols):
            cs = slice(at, at + step_cols)
            total = None
            for j in range(kw):
                term = taps_ref[j : j + 1, cs] * window[8 - kw + 1 + j : 8 - kw + 1 + j + QB, cs]
                total = term if total is None else total + term
            conv[:, cs] = silu(total)
        window[0:8, :] = window[QB : QB + 8, :]

        raw = proj_ref[here, width : width + LANES] + bias_ref[...]
        steps = jnp.maximum(raw, 0.0) + jnp.log1p(jnp.exp(-jnp.abs(raw)))
        decays = -rate_ref[...] * steps
        cum = jnp.dot(tri, decays, precision=HIGH, preferred_element_type=F32)
        cum_t = jnp.transpose(cum)
        logs[here, :] = cum + carry[0:1, :]
        carry[...] = carry[...] + cum[QB - 1 : QB, :]
        grown = jnp.exp(cum)
        tail = jnp.exp(cum[QB - 1 : QB, :] - cum)

        for g in range(groups):
            lanes = slice(g * per_group, (g + 1) * per_group)
            expand_g = expand[:, lanes]
            x = conv[:, lanes]
            b = conv[:, inner + g * N : inner + (g + 1) * N].astype(BF16)
            c = conv[:, inner + (groups + g) * N : inner + (groups + g + 1) * N].astype(BF16)
            reads[here, g * N : (g + 1) * N] = c
            scaled = x * spread_heads(steps, expand_g)
            grown_e = spread_heads(grown, expand_g)
            tailed = (scaled * spread_heads(tail, expand_g)).astype(BF16)
            scaled_low = scaled.astype(BF16)
            held = state[:, lanes]
            carried = grown_e * jnp.dot(c, held.astype(BF16), preferred_element_type=F32)
            ssd[here, lanes] = carried + skip_ref[:, lanes] * x
            fresh = lax.dot_general(
                b, tailed, (((0,), (0,)), ((), ())), preferred_element_type=F32
            )
            state[:, lanes] = grown_e[QB - 1 : QB, :] * held + fresh
            affinity = lax.dot_general(
                c, b, (((1,), (1,)), ((), ())), preferred_element_type=F32
            )
            affinity = jnp.where(causal, affinity, 0.0)
            for pair in range(per_group // LANES):
                at = pair * LANES
                inputs = scaled_low[:, at : at + LANES]
                outs = []
                for k in range(2):
                    h = (g * per_group + at) // P_SIZE + k
                    spread = jnp.minimum(cum[:, h : h + 1] - cum_t[h : h + 1, :], 0.0)
                    mixing = (affinity * jnp.exp(spread)).astype(BF16)
                    outs.append(jnp.dot(mixing, inputs, preferred_element_type=F32))
                where = slice(g * per_group + at, g * per_group + at + LANES)
                ssd[here, where] += jnp.where(low_lanes, outs[0], outs[1])
        return carry_none

    lax.fori_loop(0, blocks, block, 0)

    state_out[...] = state[...].astype(BF16)
    carry_out[...] = carry[...]

    def copies(d):
        target = lax.rem(me + d, n)
        return [
            pltpu.make_async_remote_copy(
                src_ref=source,
                dst_ref=slot.at[d - 1],
                send_sem=send_sem.at[2 * (d - 1) + k],
                recv_sem=recv_sem.at[2 * (d - 1) + k],
                device_id={"seq": target},
                device_id_type=pl.DeviceIdType.MESH,
            )
            for k, (source, slot) in enumerate(((state_out, state_in), (carry_out, carry_in)))
        ]

    for d in range(1, n):

        @pl.when(me + d < n)
        def _():
            for copy in copies(d):
                copy.start()

    state[...] = jnp.zeros_like(state)
    carry[...] = jnp.zeros_like(carry)
    for d in range(1, n):

        @pl.when(me - d >= 0)
        def _():
            for copy in copies(d):
                copy.wait_recv()
            weight = spread_heads(jnp.exp(carry[...]), expand)[0:1, :]
            state[...] += weight * state_in[d - 1].astype(F32)
            carry[...] += carry_in[d - 1]

    def finish(i, carry_none):
        here = pl.ds(pl.multiple_of(i * QB, QB), QB)
        grown = jnp.exp(logs[here, :])
        for g in range(groups):
            lanes = slice(g * per_group, (g + 1) * per_group)
            late = jnp.dot(
                reads[here, g * N : (g + 1) * N],
                state[:, lanes].astype(BF16),
                preferred_element_type=F32,
            )
            full = ssd[here, lanes] + spread_heads(grown, expand[:, lanes]) * late
            gate = proj_ref[here, gate_at + g * per_group : gate_at + (g + 1) * per_group]
            gated = full * silu(gate)
            power = jnp.mean(gated * gated, axis=-1, keepdims=True)
            y_ref[here, lanes] = (gated * lax.rsqrt(power + 1e-05) * gain_ref[:, lanes]).astype(BF16)
        return carry_none

    lax.fori_loop(0, blocks, finish, 0)
    for d in range(1, n):

        @pl.when(me + d < n)
        def _():
            for copy in copies(d):
                copy.wait_send()


def mixer(proj, rim, taps, bias, rate, skip, gain, heads, groups):
    n = lax.axis_size("seq")
    rows = proj.shape[0]
    inner = heads * P_SIZE
    width = inner + 2 * groups * N
    expand = (
        jnp.arange(LANES)[:, None] == (jnp.arange(inner) // P_SIZE)[None, :]
    ).astype(BF16)
    vmem = pl.BlockSpec(memory_space=pltpu.VMEM)
    return pl.pallas_call(
        functools.partial(mixer_kernel, n, heads, groups),
        out_shape=jax.ShapeDtypeStruct((rows, inner), BF16),
        in_specs=[vmem] * 8,
        out_specs=vmem,
        scratch_shapes=[
            pltpu.VMEM((8 + QB, width), F32),
            pltpu.VMEM((QB, width), F32),
            pltpu.VMEM((rows, inner), F32),
            pltpu.VMEM((rows, groups * N), BF16),
            pltpu.VMEM((rows, LANES), F32),
            pltpu.VMEM((N, inner), F32),
            pltpu.VMEM((8, LANES), F32),
            pltpu.VMEM((N, inner), BF16),
            pltpu.VMEM((8, LANES), F32),
            pltpu.VMEM((n - 1, N, inner), BF16),
            pltpu.VMEM((n - 1, 8, LANES), F32),
            pltpu.SemaphoreType.DMA((2 * (n - 1),)),
            pltpu.SemaphoreType.DMA((2 * (n - 1),)),
        ],
        compiler_params=pltpu.CompilerParams(
            collective_id=1, has_side_effects=True, vmem_limit_bytes=48 * 1024 * 1024
        ),
        cost_estimate=pl.CostEstimate(
            flops=8_000_000_000, bytes_accessed=100_000_000, transcendentals=8_000_000
        ),
    )(proj, rim, taps, bias, rate, skip, gain, expand)


def attention_kernel(n, rows, q_ref, k_ref, v_ref, o_ref, peak, total, acc):
    me = lax.axis_index("seq")
    reach = WINDOW // rows
    factor = HD ** (-0.5) * math.log2(math.e)
    query = q_ref[...]
    row_id = lax.broadcasted_iota(jnp.int32, (rows, rows), 0)
    col_id = lax.broadcasted_iota(jnp.int32, (rows, rows), 1)

    def visit(block, allowed, first):
        here = pl.ds(pl.multiple_of(block * rows, rows), rows)
        scores = lax.dot_general(
            query, k_ref[here, :], (((1,), (1,)), ((), ())), preferred_element_type=F32
        )
        if allowed is not None:
            scores = jnp.where(allowed, scores, -1e30)
        top = jnp.max(scores, axis=1, keepdims=True)
        if not first:
            before = peak[...]
            top = jnp.maximum(before, top)
        weights = jnp.exp2((scores - top) * factor)
        added = jnp.sum(weights, axis=1, keepdims=True)
        product = jnp.dot(weights.astype(BF16), v_ref[here, :], preferred_element_type=F32)
        if first:
            total[...] = added
            acc[...] = product
        else:
            shrink = jnp.exp2((before - top) * factor)
            total[...] = total[...] * shrink + added
            acc[...] = acc[...] * shrink + product
        peak[...] = top

    visit(me, row_id >= col_id, True)
    lowest = jnp.maximum(me - reach + 1, 0)

    def body(block, carry_none):
        visit(block, None, False)
        return carry_none

    lax.fori_loop(lowest, me, body, 0)
    if n > reach:

        @pl.when(me >= reach)
        def _():
            visit(me - reach, col_id > row_id, False)

    o_ref[...] = acc[...] / total[...]


def attention(queries, pairs, kv_heads):
    n = lax.axis_size("seq")
    rows = queries.shape[0]
    keys = pairs.shape[0]
    per_kv = queries.shape[1] // HD // kv_heads
    return pl.pallas_call(
        functools.partial(attention_kernel, n, rows),
        grid=(kv_heads, per_kv),
        out_shape=jax.ShapeDtypeStruct(queries.shape, F32),
        in_specs=[
            pl.BlockSpec((rows, HD), lambda i, j: (0, i * per_kv + j)),
            pl.BlockSpec((keys, HD), lambda i, j: (0, i)),
            pl.BlockSpec((keys, HD), lambda i, j: (0, kv_heads + i)),
        ],
        out_specs=pl.BlockSpec((rows, HD), lambda i, j: (0, i * per_kv + j)),
        scratch_shapes=[
            pltpu.VMEM((rows, 1), F32),
            pltpu.VMEM((rows, 1), F32),
            pltpu.VMEM((rows, HD), F32),
        ],
        compiler_params=pltpu.CompilerParams(
            dimension_semantics=("arbitrary", "arbitrary"), vmem_limit_bytes=40 * 1024 * 1024
        ),
        cost_estimate=pl.CostEstimate(
            flops=9_000_000_000, bytes_accessed=20_000_000, transcendentals=17_000_000
        ),
    )(queries, pairs, pairs)


def pad_lanes(values):
    return jnp.pad(values, ((0, 0), (0, LANES - values.shape[1])))


def on_device(
    hidden_in,
    norm_gain,
    w_z,
    w_x,
    w_b,
    w_c,
    w_dt,
    conv_x,
    conv_b,
    conv_c,
    dt_bias,
    a_rate,
    skip_gain,
    group_gain,
    w_out,
    attn_gain,
    w_q,
    w_k,
    w_v,
):
    whole_rows = lax.all_gather(hidden_in, "mp", axis=1, tiled=True)
    normed = rms_norm(whole_rows.astype(F32), norm_gain).astype(BF16)
    out_columns = lax.all_gather(w_out, "seq", axis=1, tiled=True)
    proj = gather_dot(
        normed, jnp.concatenate([w_x, w_b, w_c, pad_lanes(w_dt), w_z], axis=1)
    )
    heads = dt_bias.shape[0]
    groups = conv_b.shape[1] // N
    width = conv_x.shape[1] + conv_b.shape[1] + conv_c.shape[1]
    rim = from_behind(proj[proj.shape[0] - 8 :, :width], "seq", 1)
    y_normed = mixer(
        proj,
        rim,
        jnp.concatenate([conv_x, conv_b, conv_c], axis=1),
        pad_lanes(dt_bias[None, :]),
        pad_lanes(a_rate[None, :]),
        jnp.repeat(skip_gain, P_SIZE)[None, :],
        group_gain[None, :],
        heads,
        groups,
    )
    part = jnp.dot(y_normed, out_columns, preferred_element_type=F32).astype(BF16)
    summed = lax.psum_scatter(part, "mp", scatter_dimension=1, tiled=True).astype(F32)
    mixed = hidden_in.astype(F32) + summed
    mixed_low = mixed.astype(BF16)
    stream_rows = lax.all_gather(mixed_low, "mp", axis=1, tiled=True)
    normed_two = rms_norm(stream_rows.astype(F32), attn_gain).astype(BF16)
    own_keys = jnp.dot(normed_two, w_k, preferred_element_type=F32).astype(BF16)
    own_values = jnp.dot(normed_two, w_v, preferred_element_type=F32).astype(BF16)
    pairs = lax.all_gather(
        jnp.concatenate([own_keys, own_values], axis=1), "seq", axis=0, tiled=True
    )
    queries = jnp.dot(normed_two, w_q, preferred_element_type=F32).astype(BF16)
    context = attention(queries, pairs, own_keys.shape[1] // HD)
    return (mixed, context)


def solution(mesh):
    placed = (
        P("seq", "mp"),
        P(),
        P("seq", "mp"),
        P("seq", "mp"),
        P("seq", "mp"),
        P("seq", "mp"),
        P("seq", "mp"),
        P(None, "mp"),
        P(None, "mp"),
        P(None, "mp"),
        P("mp"),
        P("mp"),
        P("mp"),
        P("mp"),
        P("mp", "seq"),
        P(),
        P(None, "mp"),
        P(None, "mp"),
        P(None, "mp"),
    )
    return jax.shard_map(
        on_device,
        mesh=mesh,
        in_specs=placed,
        out_specs=(P("seq", "mp"), P("seq", "mp")),
        check_vma=False,
    )
```

```python
import functools
import math

import jax
import jax.numpy as jnp
from jax import lax
from jax.experimental import pallas as pl
from jax.experimental.pallas import tpu as pltpu
from jax.sharding import PartitionSpec as P

P_SIZE = 64
N = 128
HD = 128
WINDOW = 4096
QB = 128
LANES = 128
VMEM_LIMIT = 62 * 1024 * 1024

HIGH = lax.Precision.HIGHEST
F32 = jnp.float32
BF16 = jnp.bfloat16


def from_behind(block, axis, distance):
    devices = range(lax.axis_size(axis))
    route = [(i - distance, i) for i in devices if i - distance in devices]
    return lax.ppermute(block, axis, route)


def rms_norm(values, gain):
    return values * lax.rsqrt(jnp.mean(values * values, axis=-1, keepdims=True) + 1e-05) * gain


def signal_seq(sem, index):
    pl.semaphore_signal(
        sem, inc=1, device_id={"seq": index}, device_id_type=pl.DeviceIdType.MESH
    )


def signal_mp(sem, index):
    pl.semaphore_signal(
        sem, inc=1, device_id={"mp": index}, device_id_type=pl.DeviceIdType.MESH
    )


def norm_rows(source, gain_ref, target):
    rows = source.shape[0]
    tile = min(64, rows)

    def body(i, carry_none):
        here = pl.ds(pl.multiple_of(i * tile, tile), tile)
        target[here, :] = rms_norm(source[here, :].astype(F32), gain_ref[...]).astype(BF16)
        return carry_none

    lax.fori_loop(0, rows // tile, body, 0)


def share_features(m, source, whole, send_sem, recv_sem):
    member = lax.axis_index("mp")
    wide = source.shape[1]
    own = pl.ds(pl.multiple_of(member * wide, wide), wide)
    copies = [
        pltpu.make_async_remote_copy(
            src_ref=source,
            dst_ref=whole.at[:, own],
            send_sem=send_sem.at[d - 1],
            recv_sem=recv_sem.at[d - 1],
            device_id={"mp": lax.rem(member + d, m)},
            device_id_type=pl.DeviceIdType.MESH,
        )
        for d in range(1, m)
    ]
    for copy in copies:
        copy.start()
    return copies, own


def features_arrived(m, whole, wide, recv_sem):
    member = lax.axis_index("mp")
    for d in range(1, m):
        sender = lax.rem(member - d + m, m)
        there = whole.at[:, pl.ds(pl.multiple_of(sender * wide, wide), wide)]
        pltpu.make_async_copy(there, there, recv_sem.at[d - 1]).wait()


def gather_dot_kernel(
    n,
    m,
    hidden_ref,
    gain_ref,
    w_ref,
    out_ref,
    slots,
    normed_ref,
    local_sem,
    send_sem,
    recv_sem,
    own_sem,
    mp_send_sem,
    mp_recv_sem,
):
    me = lax.axis_index("seq")
    member = lax.axis_index("mp")
    ring = n // 2
    half = ring // 2
    chip, core = me // 2, lax.rem(me, 2)
    up = lax.rem(chip + 1, ring) * 2 + core
    down = lax.rem(chip + ring - 1, ring) * 2 + core
    partner = chip * 2 + 1 - core
    depth, cols = w_ref.shape
    mid = depth // 2

    barrier = pltpu.get_barrier_semaphore()
    for other in (up, down, partner):
        signal_seq(barrier, other)
    for d in range(1, m):
        signal_mp(barrier, lax.rem(member + d, m))
    pl.semaphore_wait(barrier, 3 + m - 1)

    shared, own = share_features(m, hidden_ref, normed_ref, mp_send_sem, mp_recv_sem)
    own_copy = pltpu.make_async_copy(hidden_ref, normed_ref.at[:, own], own_sem)
    own_copy.start()
    local = pltpu.make_async_copy(w_ref, slots.at[0], local_sem)
    local.start()
    started = []

    def send(source, slot, rows, part, target):
        copy = pltpu.make_async_remote_copy(
            src_ref=source,
            dst_ref=slots.at[slot, rows],
            send_sem=send_sem.at[len(started)],
            recv_sem=recv_sem.at[2 * slot + part],
            device_id={"seq": target},
            device_id_type=pl.DeviceIdType.MESH,
        )
        copy.start()
        started.append(copy)

    def arrived(slot, rows, part):
        pltpu.make_async_copy(
            slots.at[slot, rows], slots.at[slot, rows], recv_sem.at[2 * slot + part]
        ).wait()

    whole, upper, lower = pl.ds(0, depth), pl.ds(0, mid), pl.ds(mid, mid)
    send(w_ref, 2 * 1, whole, 0, up)
    send(w_ref, 2 * (ring - 1), whole, 0, down)
    send(w_ref, 1, whole, 0, partner)

    def multiply(slot, first=False):
        step, lane = slot // 2, slot % 2
        origin = lax.rem(chip - step + ring, ring) * 2
        owner = origin + (core if lane == 0 else 1 - core)
        features = pl.ds(pl.multiple_of(owner * depth, depth), depth)

        def tile(start, width):
            where = pl.ds(start, width)
            product = jnp.dot(
                normed_ref[:, features], slots[slot, :, where], preferred_element_type=F32
            )
            if first:
                out_ref[:, where] = product
            else:
                out_ref[:, where] += product

        width = 512
        full = cols // width

        def body(i, carry):
            tile(pl.multiple_of(i * width, width), width)
            return carry

        lax.fori_loop(0, full, body, 0)
        if cols % width:
            tile(full * width, cols % width)

    own_copy.wait()
    features_arrived(m, normed_ref, hidden_ref.shape[1], mp_recv_sem)
    norm_rows(normed_ref, gain_ref, normed_ref)
    local.wait()
    multiply(0, True)
    arrived(1, whole, 0)
    multiply(1)
    for d in range(1, half):
        s_up, s_down = 2 * d, 2 * (ring - d)
        last = d + 1 == half
        arrived(s_up, whole, 0)
        rows = upper if last else whole
        send(slots.at[s_up, rows], 2 * (d + 1), rows, 0, up)
        arrived(s_down, whole, 0)
        rows = lower if last else whole
        send(slots.at[s_down, rows], 2 * (ring - d - 1), rows, 1 if last else 0, down)
        send(slots.at[s_up, whole], s_up + 1, whole, 0, partner)
        send(slots.at[s_down, whole], s_down + 1, whole, 0, partner)
        multiply(s_up)
        multiply(s_down)
        arrived(s_up + 1, whole, 0)
        multiply(s_up + 1)
        arrived(s_down + 1, whole, 0)
        multiply(s_down + 1)
    far = 2 * half
    arrived(far, upper, 0)
    send(slots.at[far, upper], far + 1, upper, 0, partner)
    arrived(far, lower, 1)
    send(slots.at[far, lower], far + 1, lower, 1, partner)
    multiply(far)
    arrived(far + 1, upper, 0)
    arrived(far + 1, lower, 1)
    multiply(far + 1)
    for copy in started + shared:
        copy.wait_send()


def gather_dot(hidden, gain, weights):
    n, m = lax.axis_size("seq"), lax.axis_size("mp")
    depth, cols = weights.shape
    rows, features = hidden.shape[0], hidden.shape[1] * m
    ring = n // 2
    sends = 3 + 4 * (ring // 2 - 1) + 2
    return pl.pallas_call(
        functools.partial(gather_dot_kernel, n, m),
        out_shape=jax.ShapeDtypeStruct((rows, cols), F32),
        in_specs=[
            pl.BlockSpec(memory_space=pl.ANY),
            pl.BlockSpec(memory_space=pltpu.VMEM),
            pl.BlockSpec(memory_space=pl.ANY),
        ],
        out_specs=pl.BlockSpec(memory_space=pltpu.VMEM),
        scratch_shapes=[
            pltpu.VMEM((n, depth, cols), BF16),
            pltpu.VMEM((rows, features), BF16),
            pltpu.SemaphoreType.DMA,
            pltpu.SemaphoreType.DMA((sends,)),
            pltpu.SemaphoreType.DMA((2 * n,)),
            pltpu.SemaphoreType.DMA,
            pltpu.SemaphoreType.DMA((m - 1,)),
            pltpu.SemaphoreType.DMA((m - 1,)),
        ],
        compiler_params=pltpu.CompilerParams(
            collective_id=0, has_side_effects=True, vmem_limit_bytes=VMEM_LIMIT
        ),
        cost_estimate=pl.CostEstimate(
            flops=2 * rows * features * cols,
            bytes_accessed=160_000_000,
            transcendentals=0,
        ),
    )(hidden, gain, weights)


def silu(v):
    return v / (1.0 + jnp.exp(-v))


def spread_heads(values, expand):
    high = values.astype(BF16)
    low = (values - high.astype(F32)).astype(BF16)
    return jnp.dot(high, expand, preferred_element_type=F32) + jnp.dot(
        low, expand, preferred_element_type=F32
    )


def mixer_kernel(
    n,
    heads,
    groups,
    proj_ref,
    rim_ref,
    taps_ref,
    bias_ref,
    rate_ref,
    skip_ref,
    gain_ref,
    expand_ref,
    y_ref,
    window,
    conv,
    ssd,
    reads,
    logs,
    state,
    carry,
    state_out,
    carry_out,
    state_in,
    carry_in,
    send_sem,
    recv_sem,
):
    me = lax.axis_index("seq")
    rows = proj_ref.shape[0]
    inner = heads * P_SIZE
    width = inner + 2 * groups * N
    gate_at = width + LANES
    per_group = inner // groups
    blocks = rows // QB
    kw = taps_ref.shape[0]

    barrier = pltpu.get_barrier_semaphore()
    for d in range(1, n):
        signal_seq(barrier, lax.rem(me + d, n))
    pl.semaphore_wait(barrier, n - 1)

    expand = expand_ref[...]
    window[0:8, :] = rim_ref[...]
    state[...] = jnp.zeros_like(state)
    carry[...] = jnp.zeros_like(carry)
    row_id = lax.broadcasted_iota(jnp.int32, (QB, QB), 0)
    col_id = lax.broadcasted_iota(jnp.int32, (QB, QB), 1)
    causal = row_id >= col_id
    low_lanes = col_id < P_SIZE
    tri = jnp.where(causal, 1.0, 0.0).astype(F32)

    def block(i, carry_none):
        base = pl.multiple_of(i * QB, QB)
        here = pl.ds(base, QB)
        window[8 : 8 + QB, :] = proj_ref[here, 0:width]
        step_cols = 256 if width % 256 == 0 else 128
        for at in range(0, width, step_cols):
            cs = slice(at, at + step_cols)
            total = None
            for j in range(kw):
                term = taps_ref[j : j + 1, cs] * window[8 - kw + 1 + j : 8 - kw + 1 + j + QB, cs]
                total = term if total is None else total + term
            conv[:, cs] = silu(total)
        window[0:8, :] = window[QB : QB + 8, :]

        raw = proj_ref[here, width : width + LANES] + bias_ref[...]
        steps = jnp.maximum(raw, 0.0) + jnp.log1p(jnp.exp(-jnp.abs(raw)))
        decays = -rate_ref[...] * steps
        cum = jnp.dot(tri, decays, precision=HIGH, preferred_element_type=F32)
        cum_t = jnp.transpose(cum)
        logs[here, :] = cum + carry[0:1, :]
        carry[...] = carry[...] + cum[QB - 1 : QB, :]
        grown = jnp.exp(cum)
        tail = jnp.exp(cum[QB - 1 : QB, :] - cum)

        for g in range(groups):
            lanes = slice(g * per_group, (g + 1) * per_group)
            expand_g = expand[:, lanes]
            x = conv[:, lanes]
            b = conv[:, inner + g * N : inner + (g + 1) * N].astype(BF16)
            c = conv[:, inner + (groups + g) * N : inner + (groups + g + 1) * N].astype(BF16)
            reads[here, g * N : (g + 1) * N] = c
            scaled = x * spread_heads(steps, expand_g)
            grown_e = spread_heads(grown, expand_g)
            tailed = (scaled * spread_heads(tail, expand_g)).astype(BF16)
            scaled_low = scaled.astype(BF16)
            held = state[:, lanes]
            carried = grown_e * jnp.dot(c, held.astype(BF16), preferred_element_type=F32)
            ssd[here, lanes] = carried + skip_ref[:, lanes] * x
            fresh = lax.dot_general(
                b, tailed, (((0,), (0,)), ((), ())), preferred_element_type=F32
            )
            state[:, lanes] = grown_e[QB - 1 : QB, :] * held + fresh
            affinity = lax.dot_general(
                c, b, (((1,), (1,)), ((), ())), preferred_element_type=F32
            )
            affinity = jnp.where(causal, affinity, 0.0)
            for pair in range(per_group // LANES):
                at = pair * LANES
                inputs = scaled_low[:, at : at + LANES]
                outs = []
                for k in range(2):
                    h = (g * per_group + at) // P_SIZE + k
                    spread = jnp.minimum(cum[:, h : h + 1] - cum_t[h : h + 1, :], 0.0)
                    mixing = (affinity * jnp.exp(spread)).astype(BF16)
                    outs.append(jnp.dot(mixing, inputs, preferred_element_type=F32))
                where = slice(g * per_group + at, g * per_group + at + LANES)
                ssd[here, where] += jnp.where(low_lanes, outs[0], outs[1])
        return carry_none

    lax.fori_loop(0, blocks, block, 0)

    state_out[...] = state[...].astype(BF16)
    carry_out[...] = carry[...]

    def copies(d):
        target = lax.rem(me + d, n)
        return [
            pltpu.make_async_remote_copy(
                src_ref=source,
                dst_ref=slot.at[d - 1],
                send_sem=send_sem.at[2 * (d - 1) + k],
                recv_sem=recv_sem.at[2 * (d - 1) + k],
                device_id={"seq": target},
                device_id_type=pl.DeviceIdType.MESH,
            )
            for k, (source, slot) in enumerate(((state_out, state_in), (carry_out, carry_in)))
        ]

    for d in range(1, n):

        @pl.when(me + d < n)
        def _():
            for copy in copies(d):
                copy.start()

    state[...] = jnp.zeros_like(state)
    carry[...] = jnp.zeros_like(carry)
    for d in range(1, n):

        @pl.when(me - d >= 0)
        def _():
            for copy in copies(d):
                copy.wait_recv()
            weight = spread_heads(jnp.exp(carry[...]), expand)[0:1, :]
            state[...] += weight * state_in[d - 1].astype(F32)
            carry[...] += carry_in[d - 1]

    def finish(i, carry_none):
        here = pl.ds(pl.multiple_of(i * QB, QB), QB)
        grown = jnp.exp(logs[here, :])
        for g in range(groups):
            lanes = slice(g * per_group, (g + 1) * per_group)
            late = jnp.dot(
                reads[here, g * N : (g + 1) * N],
                state[:, lanes].astype(BF16),
                preferred_element_type=F32,
            )
            full = ssd[here, lanes] + spread_heads(grown, expand[:, lanes]) * late
            gate = proj_ref[here, gate_at + g * per_group : gate_at + (g + 1) * per_group]
            gated = full * silu(gate)
            power = jnp.mean(gated * gated, axis=-1, keepdims=True)
            y_ref[here, lanes] = (gated * lax.rsqrt(power + 1e-05) * gain_ref[:, lanes]).astype(BF16)
        return carry_none

    lax.fori_loop(0, blocks, finish, 0)
    for d in range(1, n):

        @pl.when(me + d < n)
        def _():
            for copy in copies(d):
                copy.wait_send()


def mixer(proj, rim, taps, bias, rate, skip, gain, heads, groups):
    n = lax.axis_size("seq")
    rows = proj.shape[0]
    inner = heads * P_SIZE
    width = inner + 2 * groups * N
    expand = (
        jnp.arange(LANES)[:, None] == (jnp.arange(inner) // P_SIZE)[None, :]
    ).astype(BF16)
    vmem = pl.BlockSpec(memory_space=pltpu.VMEM)
    return pl.pallas_call(
        functools.partial(mixer_kernel, n, heads, groups),
        out_shape=jax.ShapeDtypeStruct((rows, inner), BF16),
        in_specs=[vmem] * 8,
        out_specs=vmem,
        scratch_shapes=[
            pltpu.VMEM((8 + QB, width), F32),
            pltpu.VMEM((QB, width), F32),
            pltpu.VMEM((rows, inner), F32),
            pltpu.VMEM((rows, groups * N), BF16),
            pltpu.VMEM((rows, LANES), F32),
            pltpu.VMEM((N, inner), F32),
            pltpu.VMEM((8, LANES), F32),
            pltpu.VMEM((N, inner), BF16),
            pltpu.VMEM((8, LANES), F32),
            pltpu.VMEM((n - 1, N, inner), BF16),
            pltpu.VMEM((n - 1, 8, LANES), F32),
            pltpu.SemaphoreType.DMA((2 * (n - 1),)),
            pltpu.SemaphoreType.DMA((2 * (n - 1),)),
        ],
        compiler_params=pltpu.CompilerParams(
            collective_id=1, has_side_effects=True, vmem_limit_bytes=48 * 1024 * 1024
        ),
        cost_estimate=pl.CostEstimate(
            flops=8_000_000_000, bytes_accessed=100_000_000, transcendentals=8_000_000
        ),
    )(proj, rim, taps, bias, rate, skip, gain, expand)


def output_kernel(
    m,
    y_ref,
    w_ref,
    hidden_ref,
    gain_ref,
    mixed_ref,
    normed_ref,
    outgoing,
    incoming,
    low,
    part_send,
    part_recv,
    own_sem,
    mp_send,
    mp_recv,
):
    member = lax.axis_index("mp")
    wide = hidden_ref.shape[1]
    barrier = pltpu.get_barrier_semaphore()
    for d in range(1, m):
        signal_mp(barrier, lax.rem(member + d, m))
    pl.semaphore_wait(barrier, m - 1)
    tile = min(512, wide)

    def part(target, store):
        for at in range(0, wide, tile):
            where = pl.ds(pl.multiple_of(target * wide + at, tile), tile)
            term = jnp.dot(y_ref[...], w_ref[:, where], preferred_element_type=F32)
            store(slice(at, at + tile), term.astype(BF16))

    copies = []
    for d in range(1, m):
        target = lax.rem(member + d, m)

        def keep(where, term):
            outgoing[d - 1, :, where] = term

        part(target, keep)
        copy = pltpu.make_async_remote_copy(
            src_ref=outgoing.at[d - 1],
            dst_ref=incoming.at[d - 1],
            send_sem=part_send.at[d - 1],
            recv_sem=part_recv.at[d - 1],
            device_id={"mp": target},
            device_id_type=pl.DeviceIdType.MESH,
        )
        copy.start()
        copies.append(copy)

    def begin(where, term):
        mixed_ref[:, where] = hidden_ref[:, where].astype(F32) + term.astype(F32)

    part(member, begin)
    for d in range(1, m):
        copies[d - 1].wait_recv()
        if d < m - 1:
            mixed_ref[...] += incoming[d - 1].astype(F32)
        else:
            total = mixed_ref[...] + incoming[d - 1].astype(F32)
            mixed_ref[...] = total
            low[...] = total.astype(BF16)
    shared, own = share_features(m, low, normed_ref, mp_send, mp_recv)
    own_copy = pltpu.make_async_copy(low, normed_ref.at[:, own], own_sem)
    own_copy.start()
    own_copy.wait()
    features_arrived(m, normed_ref, wide, mp_recv)
    norm_rows(normed_ref, gain_ref, normed_ref)
    for copy in copies + shared:
        copy.wait_send()


def output_stage(y, weights, hidden, gain):
    m = lax.axis_size("mp")
    rows, wide = hidden.shape
    vmem = pl.BlockSpec(memory_space=pltpu.VMEM)
    return pl.pallas_call(
        functools.partial(output_kernel, m),
        out_shape=(
            jax.ShapeDtypeStruct((rows, wide), F32),
            jax.ShapeDtypeStruct((rows, wide * m), BF16),
        ),
        in_specs=[vmem] * 4,
        out_specs=(vmem, vmem),
        scratch_shapes=[
            pltpu.VMEM((m - 1, rows, wide), BF16),
            pltpu.VMEM((m - 1, rows, wide), BF16),
            pltpu.VMEM((rows, wide), BF16),
            pltpu.SemaphoreType.DMA((m - 1,)),
            pltpu.SemaphoreType.DMA((m - 1,)),
            pltpu.SemaphoreType.DMA,
            pltpu.SemaphoreType.DMA((m - 1,)),
            pltpu.SemaphoreType.DMA((m - 1,)),
        ],
        compiler_params=pltpu.CompilerParams(
            collective_id=2, has_side_effects=True, vmem_limit_bytes=56 * 1024 * 1024
        ),
        cost_estimate=pl.CostEstimate(
            flops=2 * rows * y.shape[1] * wide * m, bytes_accessed=60_000_000, transcendentals=0
        ),
    )(y, weights, hidden, gain)


def attention_kernel(n, rows, q_ref, k_ref, v_ref, o_ref, peak, total, acc):
    me = lax.axis_index("seq")
    reach = WINDOW // rows
    factor = HD ** (-0.5) * math.log2(math.e)
    query = q_ref[...]
    row_id = lax.broadcasted_iota(jnp.int32, (rows, rows), 0)
    col_id = lax.broadcasted_iota(jnp.int32, (rows, rows), 1)

    def visit(block, allowed, first):
        here = pl.ds(pl.multiple_of(block * rows, rows), rows)
        scores = lax.dot_general(
            query, k_ref[here, :], (((1,), (1,)), ((), ())), preferred_element_type=F32
        )
        if allowed is not None:
            scores = jnp.where(allowed, scores, -1e30)
        top = jnp.max(scores, axis=1, keepdims=True)
        if not first:
            before = peak[...]
            top = jnp.maximum(before, top)
        weights = jnp.exp2((scores - top) * factor)
        added = jnp.sum(weights, axis=1, keepdims=True)
        product = jnp.dot(weights.astype(BF16), v_ref[here, :], preferred_element_type=F32)
        if first:
            total[...] = added
            acc[...] = product
        else:
            shrink = jnp.exp2((before - top) * factor)
            total[...] = total[...] * shrink + added
            acc[...] = acc[...] * shrink + product
        peak[...] = top

    visit(me, row_id >= col_id, True)
    lowest = jnp.maximum(me - reach + 1, 0)

    def body(block, carry_none):
        visit(block, None, False)
        return carry_none

    lax.fori_loop(lowest, me, body, 0)
    if n > reach:

        @pl.when(me >= reach)
        def _():
            visit(me - reach, col_id > row_id, False)

    o_ref[...] = acc[...] / total[...]


def attention(queries, pairs, kv_heads):
    n = lax.axis_size("seq")
    rows = queries.shape[0]
    keys = pairs.shape[0]
    per_kv = queries.shape[1] // HD // kv_heads
    return pl.pallas_call(
        functools.partial(attention_kernel, n, rows),
        grid=(kv_heads, per_kv),
        out_shape=jax.ShapeDtypeStruct(queries.shape, F32),
        in_specs=[
            pl.BlockSpec((rows, HD), lambda i, j: (0, i * per_kv + j)),
            pl.BlockSpec((keys, HD), lambda i, j: (0, i)),
            pl.BlockSpec((keys, HD), lambda i, j: (0, kv_heads + i)),
        ],
        out_specs=pl.BlockSpec((rows, HD), lambda i, j: (0, i * per_kv + j)),
        scratch_shapes=[
            pltpu.VMEM((rows, 1), F32),
            pltpu.VMEM((rows, 1), F32),
            pltpu.VMEM((rows, HD), F32),
        ],
        compiler_params=pltpu.CompilerParams(
            dimension_semantics=("arbitrary", "arbitrary"), vmem_limit_bytes=40 * 1024 * 1024
        ),
        cost_estimate=pl.CostEstimate(
            flops=9_000_000_000, bytes_accessed=20_000_000, transcendentals=17_000_000
        ),
    )(queries, pairs, pairs)


def pad_lanes(values):
    return jnp.pad(values, ((0, 0), (0, LANES - values.shape[1])))


def on_device(
    hidden_in,
    norm_gain,
    w_z,
    w_x,
    w_b,
    w_c,
    w_dt,
    conv_x,
    conv_b,
    conv_c,
    dt_bias,
    a_rate,
    skip_gain,
    group_gain,
    w_out,
    attn_gain,
    w_q,
    w_k,
    w_v,
):
    proj = gather_dot(
        hidden_in,
        norm_gain[None, :],
        jnp.concatenate([w_x, w_b, w_c, pad_lanes(w_dt), w_z], axis=1),
    )
    proj, w_out = lax.optimization_barrier((proj, w_out))
    out_columns = lax.all_gather(w_out, "seq", axis=1, tiled=True)
    heads = dt_bias.shape[0]
    groups = conv_b.shape[1] // N
    width = conv_x.shape[1] + conv_b.shape[1] + conv_c.shape[1]
    rim = from_behind(proj[proj.shape[0] - 8 :, :width], "seq", 1)
    y_normed = mixer(
        proj,
        rim,
        jnp.concatenate([conv_x, conv_b, conv_c], axis=1),
        pad_lanes(dt_bias[None, :]),
        pad_lanes(a_rate[None, :]),
        jnp.repeat(skip_gain, P_SIZE)[None, :],
        group_gain[None, :],
        heads,
        groups,
    )
    mixed, normed_two = output_stage(y_normed, out_columns, hidden_in, attn_gain[None, :])
    own_keys = jnp.dot(normed_two, w_k, preferred_element_type=F32).astype(BF16)
    own_values = jnp.dot(normed_two, w_v, preferred_element_type=F32).astype(BF16)
    pairs = lax.all_gather(
        jnp.concatenate([own_keys, own_values], axis=1), "seq", axis=0, tiled=True
    )
    queries = jnp.dot(normed_two, w_q, preferred_element_type=F32).astype(BF16)
    context = attention(queries, pairs, own_keys.shape[1] // HD)
    return (mixed, context)


def solution(mesh):
    placed = (
        P("seq", "mp"),
        P(),
        P("seq", "mp"),
        P("seq", "mp"),
        P("seq", "mp"),
        P("seq", "mp"),
        P("seq", "mp"),
        P(None, "mp"),
        P(None, "mp"),
        P(None, "mp"),
        P("mp"),
        P("mp"),
        P("mp"),
        P("mp"),
        P("mp", "seq"),
        P(),
        P(None, "mp"),
        P(None, "mp"),
        P(None, "mp"),
    )
    return jax.shard_map(
        on_device,
        mesh=mesh,
        in_specs=placed,
        out_specs=(P("seq", "mp"), P("seq", "mp")),
        check_vma=False,
    )
```
